128 devices in a mesh: ep: 8 (over y, core), fs: 16 (over z, x).
Axes of the slice: x: 4, y: 4, z: 4, core: 2. Of those that a mesh axis runs over, the one named last changes fastest.
Arguments:
- grads: bfloat16 [8, 8, 256, 14336], P('ep', None, 'fs'), may hold values from -64 to 64
- counts: int32 [8, 8], replicated, may hold values from 16 to 2047
- weight: bfloat16 [8, 256, 14336], P('ep', 'fs'), may hold values from -3 to 3
- mom: float32 [8, 256, 14336], P('ep', 'fs'), may hold values from -64 to 64
- second: float32 [8, 256, 14336], P('ep', 'fs'), may hold values from 0.1 to 10
- in_weight: float32 [6, 32], replicated, may hold values from -2.5 to 2.5
- in_bias: float32 [32], replicated, may hold values from -3 to 3
- out_weight: float32 [32, 2], replicated, may hold values from -1 to 1
- out_bias: float32 [2], replicated, may hold values from -3 to 3
Outputs:
- new_weight: bfloat16 [8, 256, 14336], P('ep')
- new_mom: float32 [8, 256, 14336], P('ep', 'fs')
- new_second: float32 [8, 256, 14336], P('ep', 'fs')
The draws below stay inside these ranges and needn't reach their ends.
All inputs are finite; a program needn't handle non-finite values.
Results may differ from the reference program's by a relative error of at most 0.0019.
Values may be sent and summed in bfloat16 or wider, within the bound.
No kernel may reach another device: no remote copies, remote signals or barrier semaphores. Data moves between devices by JAX's collectives and lax.ppermute only.
A program may use at most 64 MiB of HBM per device.

```python
import math
import jax
import jax.numpy as jnp
from jax import lax

FF = 14336
EXPERTS = 8
R = 256
HID = 32
FEATS = 6


def scaled_field(key, field_shape, magnitude):
    key_noise, key_cols = jax.random.split(key, 2)
    row_scale = 10.0 ** (jnp.arange(R, dtype=jnp.float32) / R)
    col_scale = jnp.exp(jax.random.uniform(key_cols, (FF,), jnp.float32, 0.0, math.log(10.0)))
    noise_field = jnp.clip(jax.random.normal(key_noise, field_shape, jnp.float32), -6.0, 6.0)
    return magnitude * noise_field * row_scale[:, None] * col_scale


def draw_grads(key, part):
    return scaled_field(jax.random.fold_in(key, 101), (EXPERTS, EXPERTS, R, FF), 0.01).astype(jnp.bfloat16)


def draw_mom(key, part):
    return scaled_field(jax.random.fold_in(key, 202), (EXPERTS, R, FF), 0.01)


def touch_ends(array, stream_key, least, top_value):
    index_at = [jax.random.randint(jax.random.fold_in(stream_key, axis), (), 0, length) for axis, length in enumerate(array.shape)]
    longest = array.shape.index(max(array.shape))
    neighbour = index_at[:longest] + [(index_at[longest] + 1) % array.shape[longest]] + index_at[longest + 1:]
    return array.at[tuple(index_at)].set(least).at[tuple(neighbour)].set(top_value)


def level_of(rng, shape, cuts, smallest, top_value):
    factor_of = 1.0
    for position, shards_of in cuts:
        draws = jax.random.uniform(jax.random.fold_in(jax.random.fold_in(rng, 6), position), (shards_of,), jnp.float32, smallest / len(cuts), top_value / len(cuts))
        factor_of = factor_of * jnp.repeat(jnp.exp(draws), shape[position] // shards_of).reshape((-1,) + (1,) * (len(shape) - 1 - position))
    return factor_of


def noise(stream_key, shape, spread, most, cuts=(), held_as=jnp.bfloat16):
    values = jax.random.normal(stream_key, shape, jnp.float32) * spread
    if len(cuts) > 0:
        values = level_of(stream_key, shape, cuts, -0.22, 0.18) * values
    return jnp.clip(values, min=-most, max=most).astype(held_as)


def setup_inputs(seed: int = 0) -> dict:
    key_list = jax.random.split(jax.random.key(seed), 10)
    return {
        "grads": draw_grads(jax.random.fold_in(key_list[9], 71), 0),
        "counts": touch_ends(jax.random.randint(key_list[1], (EXPERTS, EXPERTS), 16, 2048), jax.random.fold_in(key_list[1], 1), 16, 2047).astype(jnp.int32),
        "weight": noise(key_list[2], (EXPERTS, R, FF), 0.5, 3.0, ((0, 8), (1, 16))),
        "mom": draw_mom(jax.random.fold_in(key_list[9], 71), 0),
        "second": jnp.clip(jnp.exp(math.log(10.0) - 4.6051702 * jax.random.uniform(key_list[4], (EXPERTS, R, FF), jnp.float32) ** level_of(key_list[4], (EXPERTS, R, FF), ((0, 8), (1, 16)), -0.2, 0.2)), 0.1, 10.0),
        "in_weight": noise(key_list[5], (FEATS, HID), FEATS ** -0.5, 2.5, (), jnp.float32),
        "in_bias": noise(key_list[6], (HID,), 0.5, 3.0, (), jnp.float32),
        "out_weight": noise(key_list[7], (HID, 2), HID ** -0.5, 1.0, (), jnp.float32),
        "out_bias": noise(key_list[8], (2,), 0.5, 3.0, (), jnp.float32),
    }


MOMENTUM_DECAY = 0.9
SECOND_DECAY = 0.99
NORM_EPS = 1e-06
ROOT_EPS = 1e-08
STEP_SCALE = 0.2
EXP_SCALE = 0.5

def learned_step(gradient, mom_next, second_next, weight, grad_norm, mom_norm, in_weight, in_bias, out_weight, out_bias):
    inv_root = lax.rsqrt(second_next + ROOT_EPS)
    features = jnp.stack([gradient / grad_norm, mom_next / mom_norm, mom_next * inv_root, gradient * inv_root, weight.astype(jnp.float32), jnp.broadcast_to(jnp.log(mom_norm), gradient.shape)])
    hidden = jax.nn.relu(jnp.einsum('fh,fab->hab', in_weight, features, precision=lax.Precision.HIGHEST) + in_bias[:, None, None])
    outputs = jnp.einsum('hk,hab->kab', out_weight, hidden, precision=lax.Precision.HIGHEST) + out_bias[:, None, None]
    update = STEP_SCALE * outputs[0] * jnp.exp(EXP_SCALE * outputs[1])
    return (weight.astype(jnp.float32) - update).astype(jnp.bfloat16)

def reference(grads, counts, weight, mom, second, in_weight, in_bias, out_weight, out_bias):
    counts_f = counts.astype(jnp.float32)
    totals = lax.optimization_barrier(jnp.sum(counts_f, axis=0))
    shares = counts_f / totals[None, :]

    def per_expert(items):
        expert_grads, expert_shares, expert_weight, expert_mom, expert_second = items
        weighted = (expert_shares[:, None, None] * expert_grads.astype(jnp.float32)).astype(jnp.bfloat16)
        weighted = lax.optimization_barrier(weighted)
        gradient = lax.optimization_barrier(jnp.sum(weighted.astype(jnp.float32), axis=0))
        mom_next = MOMENTUM_DECAY * expert_mom + (1.0 - MOMENTUM_DECAY) * gradient
        second_next = SECOND_DECAY * expert_second + (1.0 - SECOND_DECAY) * gradient * gradient
        entries = gradient.shape[0] * gradient.shape[1]
        grad_norm = jnp.sqrt(jnp.sum(gradient * gradient) / entries + NORM_EPS)
        mom_norm = jnp.sqrt(jnp.sum(mom_next * mom_next) / entries + NORM_EPS)
        updated = learned_step(gradient, mom_next, second_next, expert_weight, grad_norm, mom_norm, in_weight, in_bias, out_weight, out_bias)
        return (updated, mom_next, second_next)
    new_weight, new_mom, new_second = lax.map(per_expert, (jnp.swapaxes(grads, 0, 1), shares.T, weight, mom, second))
    return (new_weight, new_mom, new_second)
```

```python
import jax
import jax.numpy as jnp
from jax import lax
from jax.experimental import pallas as pl
from jax.experimental.pallas import tpu as pltpu
from jax.sharding import PartitionSpec as P

MOMENTUM_DECAY = 0.9
SECOND_DECAY = 0.99
NORM_EPS = 1e-06
ROOT_EPS = 1e-08
STEP_SCALE = 0.2
EXP_SCALE = 0.5
LANES = 128
COLS = 2048
CHUNK = 512


def moments_kernel(share, arrived, mom, second, gradient, mom_next, second_next, sums, acc):
    step = pl.program_id(0)

    @pl.when(step == 0)
    def _():
        acc[...] = jnp.zeros_like(acc)

    def chunk(i, carry):
        at = pl.ds(pl.multiple_of(i * CHUNK, CHUNK), CHUNK)
        grad = None
        for s in range(arrived.shape[0]):
            part = (share[s] * arrived[s, :, at].astype(jnp.float32)).astype(jnp.bfloat16)
            part = part.astype(jnp.float32)
            grad = part if grad is None else grad + part
        m = MOMENTUM_DECAY * mom[:, at] + (1.0 - MOMENTUM_DECAY) * grad
        gradient[:, at] = grad
        mom_next[:, at] = m
        second_next[:, at] = SECOND_DECAY * second[:, at] + (1.0 - SECOND_DECAY) * grad * grad
        gg, mm = grad * grad, m * m
        a, b = carry
        for k in range(0, CHUNK, LANES):
            for r in range(0, gg.shape[0], 8):
                a = a + gg[r : r + 8, k : k + LANES]
                b = b + mm[r : r + 8, k : k + LANES]
        return a, b

    a, b = lax.fori_loop(0, gradient.shape[1] // CHUNK, chunk, (acc[0], acc[1]))
    acc[0] = a
    acc[1] = b

    @pl.when(step == pl.num_programs(0) - 1)
    def _():
        sums[:, :LANES] = jnp.full((sums.shape[0], LANES), jnp.sum(a), jnp.float32)
        sums[:, LANES:] = jnp.full((sums.shape[0], LANES), jnp.sum(b), jnp.float32)


def update_kernel(
    row0, entries, in_weight, in_bias, out_weight, out_bias, sums, gradient, mom, second, weight, out, table
):
    hid = in_weight.shape[1]

    @pl.when(pl.program_id(0) == 0)
    def _():
        total = jnp.sum(sums[...], axis=0, keepdims=True)
        norm = jnp.sqrt(total / entries + NORM_EPS)
        inv = 1.0 / norm
        inv_grad = jnp.broadcast_to(inv[:, :LANES], (8, LANES))
        inv_mom = jnp.broadcast_to(inv[:, LANES:], (8, LANES))
        log_mom = jnp.broadcast_to(jnp.log(norm[:, LANES:]), (8, LANES))
        for h in range(hid):
            table[h, 0] = in_weight[0, h] * inv_grad
            table[h, 1] = in_weight[1, h] * inv_mom
            for f in (2, 3, 4):
                table[h, f] = jnp.full((8, LANES), in_weight[f, h], jnp.float32)
            table[h, 5] = in_weight[5, h] * log_mom + in_bias[h]
            table[h, 6] = jnp.full((8, LANES), out_weight[h, 0], jnp.float32)
            table[h, 7] = jnp.full((8, LANES), out_weight[h, 1], jnp.float32)

    def chunk(i, carry):
        at = pl.ds(pl.multiple_of(i * CHUNK, CHUNK), CHUNK)
        g_all, m_all = gradient[:, at], mom[:, at]
        r_all = lax.rsqrt(second[:, at] + ROOT_EPS)
        w_all = weight[row0 : row0 + 8, at].astype(jnp.float32)
        parts = [slice(k, k + LANES) for k in range(0, CHUNK, LANES)]
        g = [g_all[:, p] for p in parts]
        m = [m_all[:, p] for p in parts]
        w = [w_all[:, p] for p in parts]
        gr = [g_all[:, p] * r_all[:, p] for p in parts]
        mr = [m_all[:, p] * r_all[:, p] for p in parts]
        direction = [jnp.full((8, LANES), out_bias[0], jnp.float32) for _ in parts]
        magnitude = [jnp.full((8, LANES), out_bias[1], jnp.float32) for _ in parts]
        for h in range(hid):
            t = [table[h, f] for f in range(8)]
            for k in range(len(parts)):
                pre = (t[0] * g[k] + t[1] * m[k]) + (t[2] * mr[k] + t[3] * gr[k])
                hidden = jnp.maximum(pre + (t[4] * w[k] + t[5]), 0.0)
                direction[k] = direction[k] + t[6] * hidden
                magnitude[k] = magnitude[k] + t[7] * hidden
        new = [
            w[k] - STEP_SCALE * direction[k] * jnp.exp(EXP_SCALE * magnitude[k])
            for k in range(len(parts))
        ]
        out[:, at] = jnp.concatenate(new, axis=1).astype(jnp.bfloat16)
        return carry

    lax.fori_loop(0, out.shape[1] // CHUNK, chunk, 0)


def place_kernel(n_new, groups, *refs):
    new, out, sem = refs[:n_new], refs[-2], refs[-1]
    at = lax.axis_index("fs")
    z, x = at // 4, at % 4
    copies = []
    for n, (ref, where) in enumerate(zip(new, groups)):
        for p, (half, dz, dx, lo, hi) in enumerate(where):
            row = (((z + dz) % 4) * 4 + (x + dx) % 4) * 2 + half
            src = ref.at[p]
            dst = out.at[row] if lo is None else out.at[row, :, pl.ds(lo, hi - lo)]
            copies.append((src, dst))
    started = []
    for k, (src, dst) in enumerate(copies):
        c = pltpu.make_async_copy(src, dst, sem.at[k])
        c.start()
        started.append(c)
    for c in started:
        c.wait()


def place(into, pieces, groups, shape):
    n = sum(len(g) for g in groups)
    ins = list(pieces)
    alias = {}
    if into is not None:
        ins.append(into)
        alias = {len(ins) - 1: 0}
    return pl.pallas_call(
        lambda *refs: place_kernel(len(pieces), groups, *refs),
        out_shape=jax.ShapeDtypeStruct(shape, jnp.bfloat16),
        in_specs=[pl.BlockSpec(memory_space=pl.ANY)] * len(ins),
        out_specs=pl.BlockSpec(memory_space=pl.ANY),
        scratch_shapes=[pltpu.SemaphoreType.DMA((n,))],
        input_output_aliases=alias,
    )(*ins)


def moved(value, dz, dx):
    pairs = []
    for z in range(4):
        for x in range(4):
            pairs.append((z * 4 + x, ((z + dz) % 4) * 4 + (x + dx) % 4))
    return lax.ppermute(value, "fs", pairs)


def update_rows(row0, entries, nets, sums, gradient, mom_next, second_next, weight):
    rows, width = gradient.shape
    smem = pl.BlockSpec(memory_space=pltpu.SMEM)
    block = pl.BlockSpec((8, COLS), lambda i: (row0 // 8, i))
    return pl.pallas_call(
        lambda *refs: update_kernel(row0, entries, *refs),
        grid=(width // COLS,),
        out_shape=jax.ShapeDtypeStruct((8, width), jnp.bfloat16),
        in_specs=[smem] * 4
        + [pl.BlockSpec(sums.shape, lambda i: (0, 0)), block, block, block]
        + [pl.BlockSpec((rows, COLS), lambda i: (0, i))],
        out_specs=pl.BlockSpec((8, COLS), lambda i: (0, i)),
        scratch_shapes=[pltpu.VMEM((nets[0].shape[1], 8, 8, LANES), jnp.float32)],
    )(*nets, sums, gradient, mom_next, second_next, weight)


def per_device(grads, counts, weight, mom, second, in_weight, in_bias, out_weight, out_bias):
    rows, width = mom.shape[1:]
    sources = grads.shape[1]
    n_fs = lax.axis_size("fs")
    counts_f = counts.astype(jnp.float32)
    shares = counts_f / jnp.sum(counts_f, axis=0)
    share = lax.dynamic_index_in_dim(shares, lax.axis_index("ep"), 1, keepdims=False)
    arrived = lax.all_to_all(grads, "ep", split_axis=1, concat_axis=0, tiled=True)[:, 0]

    block = pl.BlockSpec((rows, COLS), lambda i: (0, i))
    f32 = jax.ShapeDtypeStruct((rows, width), jnp.float32)
    gradient, mom_next, second_next, sums = pl.pallas_call(
        moments_kernel,
        grid=(width // COLS,),
        out_shape=(f32, f32, f32, jax.ShapeDtypeStruct((n_fs, 2 * LANES), jnp.float32)),
        in_specs=[
            pl.BlockSpec(memory_space=pltpu.SMEM),
            pl.BlockSpec((sources, rows, COLS), lambda i: (0, 0, i)),
            block,
            block,
        ],
        out_specs=(block, block, block, pl.BlockSpec((n_fs, 2 * LANES), lambda i: (0, 0))),
        scratch_shapes=[pltpu.VMEM((2, 8, LANES), jnp.float32)],
    )(share, arrived, mom[0], second[0])

    sums = lax.all_to_all(sums, "fs", split_axis=0, concat_axis=0, tiled=True)
    entries = rows * width * n_fs
    nets = (in_weight, in_bias, out_weight, out_bias)
    top = update_rows(0, entries, nets, sums, gradient, mom_next, second_next, weight[0])
    bottom = update_rows(8, entries, nets, sums, gradient, mom_next, second_next, weight[0])

    def ring(value, cut, axis):
        go = lambda v, d: moved(v, *(d * a for a in axis))
        before = go(value, 1)
        after = go(value, -1)
        first, second_half = cut
        far = (go(first(before), 1), go(second_half(after), -1))
        return before, after, far

    by_cols = (lambda v: v[:, : width // 2], lambda v: v[:, width // 2 :])
    by_parts = (lambda v: v[:2], lambda v: v[2:])
    pieces, late, groups, late_groups = [], [], [], []
    for half, own, axis1, axis2 in ((0, top, (0, 1), (1, 0)), (1, bottom, (1, 0), (0, 1))):
        before, after, far = ring(own, by_cols, axis1)
        four = jnp.stack([own, before, after, jnp.concatenate(far, axis=1)])
        order = [0, -1, 1, 2]
        at = lambda i, j: (half, i * axis1[0] + j * axis2[0], i * axis1[1] + j * axis2[1], None, None)
        before2, after2, far2 = ring(four, by_parts, axis2)
        pieces += [four, before2, after2]
        groups += [[at(i, j) for i in order] for j in (0, -1, 1)]
        late += list(far2)
        late_groups += [[at(i, 2) for i in order[:2]], [at(i, 2) for i in order[2:]]]
    shape = (2 * n_fs, 8, width)
    out = place(None, pieces, groups, shape)
    out = place(out, late, late_groups, shape)
    return (out.reshape(1, n_fs * rows, width), mom_next[None], second_next[None])


def solution(mesh):
    in_specs = (
        P("ep", None, "fs", None),
        P(),
        P("ep", "fs", None),
        P("ep", "fs", None),
        P("ep", "fs", None),
        P(),
        P(),
        P(),
        P(),
    )
    out_specs = (P("ep", None, None), P("ep", "fs", None), P("ep", "fs", None))
    return jax.shard_map(
        per_device, mesh=mesh, in_specs=in_specs, out_specs=out_specs, check_vma=False
    )
```

```python
import jax
import jax.numpy as jnp
import numpy as np
from jax import lax
from jax.experimental import pallas as pl
from jax.experimental.pallas import tpu as pltpu
from jax.sharding import PartitionSpec as P

MOMENTUM_DECAY = 0.9
SECOND_DECAY = 0.99
NORM_EPS = 1e-06
ROOT_EPS = 1e-08
STEP_SCALE = 0.2
EXP_SCALE = 0.5
LANES = 128
CHUNK = 512
TILE = 512


def moments_kernel(share, arrived, mom, second, gradient, mom_next, second_next, sums):
    def chunk(i, carry):
        at = pl.ds(pl.multiple_of(i * CHUNK, CHUNK), CHUNK)
        grad = None
        for s in range(arrived.shape[0]):
            part = (share[s] * arrived[s, :, at].astype(jnp.float32)).astype(jnp.bfloat16)
            part = part.astype(jnp.float32)
            grad = part if grad is None else grad + part
        m = MOMENTUM_DECAY * mom[:, at] + (1.0 - MOMENTUM_DECAY) * grad
        gradient[:, at] = grad
        mom_next[:, at] = m
        second_next[:, at] = SECOND_DECAY * second[:, at] + (1.0 - SECOND_DECAY) * grad * grad
        gg, mm = grad * grad, m * m
        a, b = carry
        for k in range(0, CHUNK, LANES):
            for r in range(0, gg.shape[0], 8):
                a = a + gg[r : r + 8, k : k + LANES]
                b = b + mm[r : r + 8, k : k + LANES]
        return a, b

    zero = jnp.zeros((8, LANES), jnp.float32)
    a, b = lax.fori_loop(0, gradient.shape[1] // CHUNK, chunk, (zero, zero))
    sums[:, :4] = jnp.full((sums.shape[0], 4, LANES), jnp.sum(a), jnp.float32)
    sums[:, 4:] = jnp.full((sums.shape[0], 4, LANES), jnp.sum(b), jnp.float32)


FEATURE_OF = [0, 1, 2, 3] * 4 + [4, 4]
LOW_WEIGHT = [0] * 8 + [1] * 8 + [0, 1]
DEPTH = 8 * len(FEATURE_OF) + 16
CONSTANT_ROWS = [(5, 0), (5, 1), (6, 0), (6, 1)]


def first_layer_columns(in_weight, in_bias):
    feature = np.repeat(np.array(FEATURE_OF), 8)
    sublane = np.arange(feature.size) % 8
    feature = np.concatenate([feature, [f for f, _ in CONSTANT_ROWS]])
    seven = jnp.concatenate([in_weight, in_bias[None]])
    picked = jnp.repeat(seven[feature].T, 8, axis=0)
    mask = (np.arange(picked.shape[0])[:, None] % 8 == sublane[None]).astype(np.float32)
    mask = np.concatenate([mask, np.ones((mask.shape[0], len(CONSTANT_ROWS)), np.float32)], axis=1)
    return jnp.pad(picked * mask, ((0, 0), (0, DEPTH - feature.size)))


def update_kernel(row0, entries, out_weight, out_bias, sums, columns, gradient, mom, second, weight, out, *refs):
    layer, table = refs[-2:]
    copies = []
    if len(refs) > 2:
        mom_out, second_out, sem = refs[:3]
        copies = [pltpu.make_async_copy(mom, mom_out, sem.at[0]), pltpu.make_async_copy(second, second_out, sem.at[1])]
    for c in copies:
        c.start()
    hid = out_weight.shape[0]
    norm = jnp.sqrt(jnp.sum(sums[...], axis=0) / entries + NORM_EPS)
    inv = 1.0 / norm
    lane = lax.broadcasted_iota(jnp.int32, (1, DEPTH), 1)
    group = lane // 8
    paired = group < 16
    const0 = 8 * len(FEATURE_OF)
    is_log = (lane == const0) | (lane == const0 + 1)
    scale = jnp.where(paired & (group % 4 == 0), inv[:1, :1], 1.0)
    scale = jnp.where(paired & (group % 4 == 1), inv[4:5, :1], scale)
    scale = jnp.where(is_log, jnp.log(norm[4:5, :1]), scale)
    low = ((group >= 8) & paired) | (group == 17)
    low = low | ((lane >= const0) & (lane % 2 == 1))
    full = columns[...] * scale
    high = full.astype(jnp.bfloat16).astype(jnp.float32)
    layer[...] = jnp.where(low, full - high, high).astype(jnp.bfloat16)
    for h in range(hid):
        table[h, 0] = jnp.full((8, LANES), out_weight[h, 0], jnp.float32)
        table[h, 1] = jnp.full((8, LANES), out_weight[h, 1], jnp.float32)

    def split(pair):
        both = jnp.concatenate(pair, axis=0)
        high = both.astype(jnp.bfloat16)
        return high, (both - high.astype(jnp.float32)).astype(jnp.bfloat16)

    def chunk(i, carry):
        at = pl.ds(pl.multiple_of(i * TILE, TILE), TILE)
        g, m = gradient[row0 : row0 + 8, at], mom[row0 : row0 + 8, at]
        r = lax.rsqrt(second[row0 : row0 + 8, at] + ROOT_EPS)
        w = weight[row0 : row0 + 8, at].astype(jnp.float32)
        high1, low1 = split([g, m])
        high2, low2 = split([m * r, g * r])
        last = jnp.concatenate([w, w], axis=0).astype(jnp.bfloat16)
        ones = jnp.ones((16, TILE), jnp.bfloat16)
        rows = jnp.concatenate([high1, high2, low1, low2, high1, high2, low1, low2, last, ones], axis=0)
        pre = jnp.dot(layer[...], rows, preferred_element_type=jnp.float32)
        parts = [slice(k, k + LANES) for k in range(0, TILE, LANES)]
        direction = [jnp.full((8, LANES), out_bias[0], jnp.float32) for _ in parts]
        magnitude = [jnp.full((8, LANES), out_bias[1], jnp.float32) for _ in parts]
        for h in range(hid):
            t0, t1 = table[h, 0], table[h, 1]
            for k, p in enumerate(parts):
                hidden = jnp.maximum(pre[8 * h : 8 * h + 8, p], 0.0)
                direction[k] = direction[k] + t0 * hidden
                magnitude[k] = magnitude[k] + t1 * hidden
        direction = jnp.concatenate(direction, axis=1)
        magnitude = jnp.concatenate(magnitude, axis=1)
        out[:, at] = (w - STEP_SCALE * direction * jnp.exp(EXP_SCALE * magnitude)).astype(jnp.bfloat16)
        return carry

    lax.fori_loop(0, out.shape[1] // TILE, chunk, 0)
    for c in copies:
        c.wait()


def here(value):
    return pltpu.with_memory_space_constraint(value, pltpu.VMEM)


def place_kernel(n_new, groups, *refs):
    new, out, sem = refs[:n_new], refs[-2], refs[-1]
    at = lax.axis_index("fs")
    z, x = at // 4, at % 4
    copies = []
    for n, (ref, where) in enumerate(zip(new, groups)):
        for p, (half, dz, dx, lo, hi) in enumerate(where):
            row = (((z + dz) % 4) * 4 + (x + dx) % 4) * 2 + half
            src = ref.at[p]
            dst = out.at[row] if lo is None else out.at[row, :, pl.ds(lo, hi - lo)]
            copies.append((src, dst))
    started = []
    for k, (src, dst) in enumerate(copies):
        c = pltpu.make_async_copy(src, dst, sem.at[k])
        c.start()
        started.append(c)
    for c in started:
        c.wait()


def place(into, pieces, groups, shape):
    n = sum(len(g) for g in groups)
    ins = [pltpu.with_memory_space_constraint(p, pltpu.VMEM) for p in pieces]
    specs = [pl.BlockSpec(memory_space=pltpu.VMEM)] * len(ins)
    alias = {}
    if into is not None:
        ins.append(into)
        specs.append(pl.BlockSpec(memory_space=pl.ANY))
        alias = {len(ins) - 1: 0}
    return pl.pallas_call(
        lambda *refs: place_kernel(len(pieces), groups, *refs),
        out_shape=jax.ShapeDtypeStruct(shape, jnp.bfloat16),
        in_specs=specs,
        out_specs=pl.BlockSpec(memory_space=pl.ANY),
        scratch_shapes=[pltpu.SemaphoreType.DMA((n,))],
        compiler_params=pltpu.CompilerParams(vmem_limit_bytes=1 << 20),
        input_output_aliases=alias,
    )(*ins)


def moved(value, dz, dx):
    pairs = []
    for z in range(4):
        for x in range(4):
            pairs.append((z * 4 + x, ((z + dz) % 4) * 4 + (x + dx) % 4))
    return lax.ppermute(value, "fs", pairs)


def update_rows(row0, entries, out_weight, out_bias, sums, columns, gradient, mom_next, second_next, weight):
    rows, width = gradient.shape
    smem = pl.BlockSpec(memory_space=pltpu.SMEM)
    vmem = pl.BlockSpec(memory_space=pltpu.VMEM)
    arrays = [here(v) for v in (sums, columns, gradient, mom_next, second_next, weight)]
    outs, out_specs, sems = [pltpu.VMEM((8, width), jnp.bfloat16)], [vmem], []
    if row0 == 0:
        outs += [jax.ShapeDtypeStruct(v.shape, v.dtype) for v in (mom_next, second_next)]
        out_specs += [pl.BlockSpec(memory_space=pl.ANY)] * 2
        sems = [pltpu.SemaphoreType.DMA((2,))]

    return pl.pallas_call(
        lambda *refs: update_kernel(row0, entries, *refs),
        out_shape=tuple(outs),
        in_specs=[smem] * 2 + [vmem] * len(arrays),
        out_specs=tuple(out_specs),
        scratch_shapes=sems
        + [
            pltpu.VMEM(columns.shape, jnp.bfloat16),
            pltpu.VMEM((out_weight.shape[0], 2, 8, LANES), jnp.float32),
        ],
        compiler_params=pltpu.CompilerParams(vmem_limit_bytes=8 << 20),
    )(out_weight, out_bias, *arrays)


def per_device(grads, counts, weight, mom, second, in_weight, in_bias, out_weight, out_bias):
    rows, width = mom.shape[1:]
    sources = grads.shape[1]
    n_fs = lax.axis_size("fs")
    counts_f = counts.astype(jnp.float32)
    shares = counts_f / jnp.sum(counts_f, axis=0)
    share = lax.dynamic_index_in_dim(shares, lax.axis_index("ep"), 1, keepdims=False)
    arrived = lax.all_to_all(grads, "ep", split_axis=1, concat_axis=0, tiled=True)[:, 0]

    columns = first_layer_columns(in_weight, in_bias)
    vmem = pl.BlockSpec(memory_space=pltpu.VMEM)
    f32 = pltpu.VMEM((rows, width), jnp.float32)
    gradient, mom_next, second_next, sums = pl.pallas_call(
        moments_kernel,
        out_shape=(f32, f32, f32, pltpu.VMEM((n_fs, 8, LANES), jnp.float32)),
        in_specs=[pl.BlockSpec(memory_space=pltpu.SMEM), vmem, vmem, vmem],
        out_specs=(vmem, vmem, vmem, vmem),
        compiler_params=pltpu.CompilerParams(vmem_limit_bytes=4 << 20),
    )(share, here(arrived), here(mom[0]), here(second[0]))

    sums = lax.all_to_all(sums, "fs", split_axis=0, concat_axis=0, tiled=True)
    entries = rows * width * n_fs
    args = (entries, out_weight, out_bias, sums, columns, gradient, mom_next, second_next, weight[0])
    top, mom_next, second_next = update_rows(0, *args)
    (bottom,) = update_rows(8, *args)

    def ring(value, cut, axis):
        go = lambda v, d: moved(v, *(d * a for a in axis))
        before = go(value, 1)
        after = go(value, -1)
        first, second_half = cut
        far = (go(first(before), 1), go(second_half(after), -1))
        return before, after, far

    by_cols = (lambda v: v[:, : width // 2], lambda v: v[:, width // 2 :])
    by_parts = (lambda v: v[:2], lambda v: v[2:])
    pieces, late, groups, late_groups = [], [], [], []
    for half, own, axis1, axis2 in ((0, top, (0, 1), (1, 0)), (1, bottom, (1, 0), (0, 1))):
        before, after, far = ring(own, by_cols, axis1)
        four = jnp.stack([own, before, after, jnp.concatenate(far, axis=1)])
        order = [0, -1, 1, 2]
        at = lambda i, j: (half, i * axis1[0] + j * axis2[0], i * axis1[1] + j * axis2[1], None, None)
        before2, after2, far2 = ring(four, by_parts, axis2)
        pieces += [four, before2, after2]
        groups += [[at(i, j) for i in order] for j in (0, -1, 1)]
        late += list(far2)
        late_groups += [[at(i, 2) for i in order[:2]], [at(i, 2) for i in order[2:]]]
    shape = (2 * n_fs, 8, width)
    out = place(None, pieces, groups, shape)
    out = place(out, late, late_groups, shape)
    return (out.reshape(1, n_fs * rows, width), mom_next[None], second_next[None])


def solution(mesh):
    in_specs = (
        P("ep", None, "fs", None),
        P(),
        P("ep", "fs", None),
        P("ep", "fs", None),
        P("ep", "fs", None),
        P(),
        P(),
        P(),
        P(),
    )
    out_specs = (P("ep", None, None), P("ep", "fs", None), P("ep", "fs", None))
    return jax.shard_map(
        per_device, mesh=mesh, in_specs=in_specs, out_specs=out_specs, check_vma=False
    )
```

```python
import jax
import jax.numpy as jnp
import numpy as np
from jax import lax
from jax.experimental import pallas as pl
from jax.experimental.pallas import tpu as pltpu
from jax.sharding import PartitionSpec as P

MOMENTUM_DECAY = 0.9
SECOND_DECAY = 0.99
NORM_EPS = 1e-06
ROOT_EPS = 1e-08
STEP_SCALE = 0.2
EXP_SCALE = 0.5
LANES = 128
COLS = 2048
CHUNK = 512
TILE = 512


def moments_kernel(
    scalars, columns_in, arrived, mom, second, weight,
    gradient, mom_next, second_next, weight_here, sums, table, columns, buffer, sem,
):
    width = gradient.shape[1]
    sources = arrived.shape[0]
    copies = []
    for k in range(width // COLS):
        at = pl.ds(k * COLS, COLS)
        three = [
            (arrived.at[:, :, at], buffer.at[:, :, at]),
            (mom.at[:, at], mom_next.at[:, at]),
            (second.at[:, at], second_next.at[:, at]),
        ]
        copies.append([pltpu.make_async_copy(*pair, sem.at[k, j]) for j, pair in enumerate(three)])
        for c in copies[-1]:
            c.start()
    last = pltpu.make_async_copy(weight, weight_here, sem.at[width // COLS, 0])
    last.start()
    for h in range(table.shape[0]):
        for j in range(2):
            table[h, j] = jnp.full((8, LANES), scalars[sources + 2 * h + j], jnp.float32)
    columns[...] = columns_in[...]

    def chunk(i, carry):
        at = pl.ds(pl.multiple_of(i * CHUNK, CHUNK), CHUNK)
        grad = None
        for s in range(sources):
            part = (scalars[s] * buffer[s, :, at].astype(jnp.float32)).astype(jnp.bfloat16)
            part = part.astype(jnp.float32)
            grad = part if grad is None else grad + part
        m = MOMENTUM_DECAY * mom_next[:, at] + (1.0 - MOMENTUM_DECAY) * grad
        gradient[:, at] = grad
        mom_next[:, at] = m
        second_next[:, at] = SECOND_DECAY * second_next[:, at] + (1.0 - SECOND_DECAY) * grad * grad
        gg, mm = grad * grad, m * m
        a, b = carry
        for k in range(0, CHUNK, LANES):
            for r in range(0, gg.shape[0], 8):
                a = a + gg[r : r + 8, k : k + LANES]
                b = b + mm[r : r + 8, k : k + LANES]
        return a, b

    zero = jnp.zeros((8, LANES), jnp.float32)
    carry = (zero, zero)
    per = COLS // CHUNK
    for k, three in enumerate(copies):
        for c in three:
            c.wait()
        carry = lax.fori_loop(k * per, (k + 1) * per, chunk, carry)
    a, b = carry
    sums[:, :4] = jnp.full((sums.shape[0], 4, LANES), jnp.sum(a), jnp.float32)
    sums[:, 4:] = jnp.full((sums.shape[0], 4, LANES), jnp.sum(b), jnp.float32)
    last.wait()


FEATURE_OF = [0, 1, 2, 3] * 4 + [4, 4]
LOW_WEIGHT = [0] * 8 + [1] * 8 + [0, 1]
DEPTH = 8 * len(FEATURE_OF) + 16
CONSTANT_ROWS = [(5, 0), (5, 1), (6, 0), (6, 1)]


def first_layer_columns(in_weight, in_bias):
    feature = np.repeat(np.array(FEATURE_OF), 8)
    sublane = np.arange(feature.size) % 8
    feature = np.concatenate([feature, [f for f, _ in CONSTANT_ROWS]])
    seven = jnp.concatenate([in_weight, in_bias[None]])
    picked = jnp.repeat(seven[feature].T, 8, axis=0)
    mask = (np.arange(picked.shape[0])[:, None] % 8 == sublane[None]).astype(np.float32)
    mask = np.concatenate([mask, np.ones((mask.shape[0], len(CONSTANT_ROWS)), np.float32)], axis=1)
    return jnp.pad(picked * mask, ((0, 0), (0, DEPTH - feature.size)))


def update_kernel(row0, entries, sums, table, columns, gradient, mom, second, weight, out, *refs):
    layer, pre0, pre1 = refs[-3:]
    copies = []
    if len(refs) > 3:
        mom_out, second_out, sem = refs[:3]
        copies = [pltpu.make_async_copy(mom, mom_out, sem.at[0]), pltpu.make_async_copy(second, second_out, sem.at[1])]
    for c in copies:
        c.start()
    hid = table.shape[0] - 1
    norm = jnp.sqrt(jnp.sum(sums[...], axis=0) / entries + NORM_EPS)
    inv = 1.0 / norm
    lane = lax.broadcasted_iota(jnp.int32, (1, DEPTH), 1)
    group = lane // 8
    paired = group < 16
    const0 = 8 * len(FEATURE_OF)
    is_log = (lane == const0) | (lane == const0 + 1)
    scale = jnp.where(paired & (group % 4 == 0), inv[:1, :1], 1.0)
    scale = jnp.where(paired & (group % 4 == 1), inv[4:5, :1], scale)
    scale = jnp.where(is_log, jnp.log(norm[4:5, :1]), scale)
    low = ((group >= 8) & paired) | (group == 17)
    low = low | ((lane >= const0) & (lane % 2 == 1))
    full = columns[...] * scale
    high = full.astype(jnp.bfloat16).astype(jnp.float32)
    layer[...] = jnp.where(low, full - high, high).astype(jnp.bfloat16)

    def split(pair):
        both = jnp.concatenate(pair, axis=0)
        high = both.astype(jnp.bfloat16)
        return high, (both - high.astype(jnp.float32)).astype(jnp.bfloat16)

    def first(i, pre):
        at = pl.ds(pl.multiple_of(i * TILE, TILE), TILE)
        g, m = gradient[row0 : row0 + 8, at], mom[row0 : row0 + 8, at]
        r = lax.rsqrt(second[row0 : row0 + 8, at] + ROOT_EPS)
        w = weight[row0 : row0 + 8, at].astype(jnp.float32)
        high1, low1 = split([g, m])
        high2, low2 = split([m * r, g * r])
        last = jnp.concatenate([w, w], axis=0).astype(jnp.bfloat16)
        ones = jnp.ones((16, TILE), jnp.bfloat16)
        rows = jnp.concatenate([high1, high2, low1, low2, high1, high2, low1, low2, last, ones], axis=0)
        pre[...] = jnp.dot(layer[...], rows, preferred_element_type=jnp.float32)

    def rest(i, pre):
        at = pl.ds(pl.multiple_of(i * TILE, TILE), TILE)
        parts = [slice(k, k + LANES) for k in range(0, TILE, LANES)]
        direction = [table[hid, 0] for _ in parts]
        magnitude = [table[hid, 1] for _ in parts]
        for h in range(hid):
            t0, t1 = table[h, 0], table[h, 1]
            for k, p in enumerate(parts):
                hidden = jnp.maximum(pre[8 * h : 8 * h + 8, p], 0.0)
                direction[k] = direction[k] + t0 * hidden
                magnitude[k] = magnitude[k] + t1 * hidden
        direction = jnp.concatenate(direction, axis=1)
        magnitude = jnp.concatenate(magnitude, axis=1)
        w = weight[row0 : row0 + 8, at].astype(jnp.float32)
        out[:, at] = (w - STEP_SCALE * direction * jnp.exp(EXP_SCALE * magnitude)).astype(jnp.bfloat16)

    tiles = out.shape[1] // TILE
    first(0, pre0)

    def two(i, carry):
        first(2 * i + 1, pre1)
        rest(2 * i, pre0)
        first(jnp.minimum(2 * i + 2, tiles - 1), pre0)
        rest(2 * i + 1, pre1)
        return carry

    lax.fori_loop(0, tiles // 2, two, 0)
    for c in copies:
        c.wait()


def here(value):
    return pltpu.with_memory_space_constraint(value, pltpu.VMEM)


def place_kernel(spots, *refs):
    out, sem = refs[-2], refs[-1]
    at = lax.axis_index("fs")
    z, x = at // 4, at % 4
    copies = []
    for ref, where in zip(refs, spots):
        for p, (half, dz, dx) in enumerate(where):
            row = (((z + dz) % 4) * 4 + (x + dx) % 4) * 2 + half
            src = ref if len(where) == 1 else ref.at[p]
            copies.append(pltpu.make_async_copy(src, out.at[row], sem.at[len(copies)]))
            copies[-1].start()
    for c in copies:
        c.wait()


def place(into, pieces, shape):
    ins = [here(p) for p, _ in pieces]
    specs = [pl.BlockSpec(memory_space=pltpu.VMEM)] * len(ins)
    alias = {}
    if into is not None:
        ins.append(into)
        specs.append(pl.BlockSpec(memory_space=pl.ANY))
        alias = {len(ins) - 1: 0}
    spots = [spot for _, spot in pieces]
    return pl.pallas_call(
        lambda *refs: place_kernel(spots, *refs),
        out_shape=jax.ShapeDtypeStruct(shape, jnp.bfloat16),
        in_specs=specs,
        out_specs=pl.BlockSpec(memory_space=pl.ANY),
        scratch_shapes=[pltpu.SemaphoreType.DMA((sum(map(len, spots)),))],
        compiler_params=pltpu.CompilerParams(vmem_limit_bytes=1 << 20),
        input_output_aliases=alias,
    )(*ins)


def moved(value, dz, dx):
    pairs = []
    for z in range(4):
        for x in range(4):
            pairs.append((z * 4 + x, ((z + dz) % 4) * 4 + (x + dx) % 4))
    return lax.ppermute(value, "fs", pairs)


def update_rows(row0, entries, sums, table, columns, gradient, mom_next, second_next, weight):
    rows, width = gradient.shape
    vmem = pl.BlockSpec(memory_space=pltpu.VMEM)
    arrays = [here(v) for v in (sums, table, columns, gradient, mom_next, second_next, weight)]
    outs, out_specs, sems = [pltpu.VMEM((8, width), jnp.bfloat16)], [vmem], []
    if row0 == 0:
        outs += [jax.ShapeDtypeStruct(v.shape, v.dtype) for v in (mom_next, second_next)]
        out_specs += [pl.BlockSpec(memory_space=pl.ANY)] * 2
        sems = [pltpu.SemaphoreType.DMA((2,))]

    return pl.pallas_call(
        lambda *refs: update_kernel(row0, entries, *refs),
        out_shape=tuple(outs),
        in_specs=[vmem] * len(arrays),
        out_specs=tuple(out_specs),
        scratch_shapes=sems
        + [
            pltpu.VMEM(columns.shape, jnp.bfloat16),
            pltpu.VMEM((columns.shape[0], TILE), jnp.float32),
            pltpu.VMEM((columns.shape[0], TILE), jnp.float32),
        ],
        compiler_params=pltpu.CompilerParams(vmem_limit_bytes=8 << 20),
    )(*arrays)


def per_device(grads, counts, weight, mom, second, in_weight, in_bias, out_weight, out_bias):
    rows, width = mom.shape[1:]
    sources = grads.shape[1]
    n_fs = lax.axis_size("fs")
    counts_f = counts.astype(jnp.float32)
    shares = counts_f / jnp.sum(counts_f, axis=0)
    share = lax.dynamic_index_in_dim(shares, lax.axis_index("ep"), 1, keepdims=False)
    arrived = lax.all_to_all(grads, "ep", split_axis=1, concat_axis=0, tiled=True)[:, 0]

    columns = first_layer_columns(in_weight, in_bias)
    vmem, hbm = pl.BlockSpec(memory_space=pltpu.VMEM), pl.BlockSpec(memory_space=pl.ANY)
    f32 = pltpu.VMEM((rows, width), jnp.float32)
    hid = out_weight.shape[0]
    scalars = jnp.concatenate([share, out_weight.reshape(-1), out_bias])
    gradient, mom_next, second_next, weight_here, sums, table, columns = pl.pallas_call(
        moments_kernel,
        out_shape=(
            f32,
            f32,
            f32,
            pltpu.VMEM((rows, width), jnp.bfloat16),
            pltpu.VMEM((n_fs, 8, LANES), jnp.float32),
            pltpu.VMEM((hid + 1, 2, 8, LANES), jnp.float32),
            pltpu.VMEM(columns.shape, jnp.float32),
        ),
        in_specs=[pl.BlockSpec(memory_space=pltpu.SMEM), vmem, hbm, hbm, hbm, hbm],
        out_specs=(vmem,) * 7,
        scratch_shapes=[
            pltpu.VMEM((sources, rows, width), jnp.bfloat16),
            pltpu.SemaphoreType.DMA((width // COLS + 1, 3)),
        ],
        compiler_params=pltpu.CompilerParams(vmem_limit_bytes=6 << 20),
    )(scalars, columns, arrived, mom[0], second[0], weight[0])

    sums = lax.all_to_all(sums, "fs", split_axis=0, concat_axis=0, tiled=True)
    entries = rows * width * n_fs
    args = (entries, sums, table, columns, gradient, mom_next, second_next, weight_here)
    top, mom_next, second_next = update_rows(0, *args)
    (bottom,) = update_rows(8, *args)

    def go(value, axis, d):
        return moved(value, *(d * a for a in axis))

    halves = ((0, top, (0, 1), (1, 0)), (1, bottom, (1, 0), (0, 1)))
    stages = [[], [], []]
    for half, own, along, across in halves:
        at = lambda i, j: (half, i * along[0] + j * across[0], i * along[1] + j * across[1])
        before, after = go(own, along, 1), go(own, along, -1)
        both = jnp.stack([before, after])
        far = go(before, along, 1)
        line = [(own, (0,)), (both, (-1, 1)), (far, (2,))]
        for n, (part, where) in enumerate(line):
            below, above = go(part, across, 1), go(part, across, -1)
            beyond = go(below, across, 1) if n == 1 else go(above, across, -1)
            spots = lambda j: [at(i, j) for i in where]
            stages[0].append((part, spots(0)))
            stages[min(n, 1)] += [(below, spots(-1)), (above, spots(1))]
            stages[2 if n == 2 else 1].append((beyond, spots(2)))
    shape = (2 * n_fs, 8, width)
    out = None
    for pieces in stages:
        out = place(out, pieces, shape)
    return (out.reshape(1, n_fs * rows, width), mom_next[None], second_next[None])


def solution(mesh):
    in_specs = (
        P("ep", None, "fs", None),
        P(),
        P("ep", "fs", None),
        P("ep", "fs", None),
        P("ep", "fs", None),
        P(),
        P(),
        P(),
        P(),
    )
    out_specs = (P("ep", None, None), P("ep", "fs", None), P("ep", "fs", None))
    return jax.shard_map(
        per_device, mesh=mesh, in_specs=in_specs, out_specs=out_specs, check_vma=False
    )
```

```python
import jax
import jax.numpy as jnp
import numpy as np
from jax import lax
from jax.experimental import pallas as pl
from jax.experimental.pallas import tpu as pltpu
from jax.sharding import PartitionSpec as P


MOMENTUM_DECAY = 0.9
SECOND_DECAY = 0.99
NORM_EPS = 1e-06
ROOT_EPS = 1e-08
STEP_SCALE = 0.2
EXP_SCALE = 0.5
LANES = 128
CHUNK = 2048
TILE = 1024


SENDS = [[(2, 0)], [(1, 0), (-1, 0)], [(2, 1), (1, 1)], [(-1, 1), (0, 1), (0, 0)]]
EARLY = [(0, 0), (2, 0), (2, 1), (0, 1), (1, 0), (-1, 0)]
LATE = [(1, 1), (-1, 1)]


def peer(ep, dy, dc, cores=2):
    chips = lax.axis_size("ep") // cores
    return (ep // cores + dy) % chips * cores + (ep % cores + dc) % cores


def weighted_sum(scalars, slots, parts, at, start=None):
    ep = lax.axis_index("ep")
    for (dy, dc), part in zip(slots, parts):
        share = scalars[peer(ep, -dy, dc)]
        term = (share * part[:, at].astype(jnp.float32)).astype(jnp.bfloat16).astype(jnp.float32)
        start = term if start is None else start + term
    return start


def early_kernel(scalars, columns_in, mom, second, weight, *refs):
    parts = refs[: len(EARLY)]
    total, mom_here, second_here, weight_here, table, columns, sem = refs[len(EARLY) :]
    pairs = [(mom, mom_here), (second, second_here), (weight, weight_here)]
    copies = [pltpu.make_async_copy(src, dst, sem.at[k]) for k, (src, dst) in enumerate(pairs)]
    for c in copies:
        c.start()
    first = lax.axis_size("ep")
    for h in range(table.shape[0]):
        for j in range(2):
            table[h, j] = jnp.full((8, LANES), scalars[first + 2 * h + j], jnp.float32)
    columns[...] = columns_in[...]

    def chunk(i, carry):
        at = pl.ds(pl.multiple_of(i * CHUNK, CHUNK), CHUNK)
        total[:, at] = weighted_sum(scalars, EARLY, parts, at)
        return carry

    lax.fori_loop(0, total.shape[1] // CHUNK, chunk, 0)
    for c in copies:
        c.wait()


def folded(squares):
    tiles = [
        squares[r : r + 8, k : k + LANES]
        for k in range(0, squares.shape[1], LANES)
        for r in range(0, squares.shape[0], 8)
    ]
    while len(tiles) > 1:
        tiles = [a + b for a, b in zip(tiles[::2], tiles[1::2])] + tiles[len(tiles) // 2 * 2 :]
    return tiles[0]


def moments_kernel(scalars, early, mom, second, *refs):
    parts = refs[: len(LATE)]
    gradient, mom_next, second_next, sums = refs[len(LATE) :]

    def chunk(i, carry):
        at = pl.ds(pl.multiple_of(i * CHUNK, CHUNK), CHUNK)
        grad = weighted_sum(scalars, LATE, parts, at, early[:, at])
        m = MOMENTUM_DECAY * mom[:, at] + (1.0 - MOMENTUM_DECAY) * grad
        gradient[:, at] = grad
        mom_next[:, at] = m
        second_next[:, at] = SECOND_DECAY * second[:, at] + (1.0 - SECOND_DECAY) * grad * grad
        gg, mm = grad * grad, m * m
        return carry[0] + folded(gg), carry[1] + folded(mm)

    zero = jnp.zeros((8, LANES), jnp.float32)
    a, b = lax.fori_loop(0, gradient.shape[1] // CHUNK, chunk, (zero, zero))
    sums[:, :4] = jnp.full((sums.shape[0], 4, LANES), jnp.sum(a), jnp.float32)
    sums[:, 4:] = jnp.full((sums.shape[0], 4, LANES), jnp.sum(b), jnp.float32)


FEATURE_OF = [0, 1, 2, 3] * 4 + [4, 4]
DEPTH = 8 * len(FEATURE_OF) + 16
CONSTANT_ROWS = [(5, 0), (5, 1), (6, 0), (6, 1)]


def first_layer_columns(in_weight, in_bias):
    feature = np.repeat(np.array(FEATURE_OF), 8)
    sublane = np.arange(feature.size) % 8
    feature = np.concatenate([feature, [f for f, _ in CONSTANT_ROWS]])
    seven = jnp.concatenate([in_weight, in_bias[None]])
    picked = jnp.repeat(seven[feature].T, 8, axis=0)
    mask = (np.arange(picked.shape[0])[:, None] % 8 == sublane[None]).astype(np.float32)
    mask = np.concatenate([mask, np.ones((mask.shape[0], len(CONSTANT_ROWS)), np.float32)], axis=1)
    return jnp.pad(picked * mask, ((0, 0), (0, DEPTH - feature.size)))


def update_kernel(row0, entries, sums, table, columns, gradient, mom, second, weight, *refs):
    hid = table.shape[0] - 1
    pre0, pre1 = refs[-2:]
    copies = []
    if row0 == 0:
        out, layer, mom_out, second_out, sem = refs[:5]
        copies = [pltpu.make_async_copy(mom, mom_out, sem.at[0]), pltpu.make_async_copy(second, second_out, sem.at[1])]
    else:
        layer, out = refs[:2]
    for c in copies:
        c.start()
    if row0 == 0:
        norm = jnp.sqrt(jnp.sum(sums[...], axis=0) / entries + NORM_EPS)
        inv = 1.0 / norm
        lane = lax.broadcasted_iota(jnp.int32, (1, DEPTH), 1)
        group = lane // 8
        paired = group < 16
        const0 = 8 * len(FEATURE_OF)
        is_log = (lane == const0) | (lane == const0 + 1)
        scale = jnp.where(paired & (group % 4 == 0), inv[:1, :1], 1.0)
        scale = jnp.where(paired & (group % 4 == 1), inv[4:5, :1], scale)
        scale = jnp.where(is_log, jnp.log(norm[4:5, :1]), scale)
        low = ((group >= 8) & paired) | (group == 17)
        low = low | ((lane >= const0) & (lane % 2 == 1))
        full = columns[...] * scale
        high = full.astype(jnp.bfloat16).astype(jnp.float32)
        layer[...] = jnp.where(low, full - high, high).astype(jnp.bfloat16)

    def split(pair):
        both = jnp.concatenate(pair, axis=0)
        high = both.astype(jnp.bfloat16)
        return high, (both - high.astype(jnp.float32)).astype(jnp.bfloat16)

    def first(i, pre):
        at = pl.ds(pl.multiple_of(i * TILE, TILE), TILE)
        g, m = gradient[row0 : row0 + 8, at], mom[row0 : row0 + 8, at]
        r = lax.rsqrt(second[row0 : row0 + 8, at] + ROOT_EPS)
        w = weight[row0 : row0 + 8, at].astype(jnp.float32)
        high1, low1 = split([g, m])
        high2, low2 = split([m * r, g * r])
        last = jnp.concatenate([w, w], axis=0).astype(jnp.bfloat16)
        ones = jnp.ones((16, TILE), jnp.bfloat16)
        rows = jnp.concatenate([high1, high2, low1, low2, high1, high2, low1, low2, last, ones], axis=0)
        pre[...] = jnp.dot(layer[...], rows, preferred_element_type=jnp.float32)

    def rest(i, pre):
        at = pl.ds(pl.multiple_of(i * TILE, TILE), TILE)
        parts = [slice(k, k + LANES) for k in range(0, TILE, LANES)]
        direction = [table[hid, 0] for _ in parts]
        magnitude = [table[hid, 1] for _ in parts]
        for h in range(hid):
            t0, t1 = table[h, 0], table[h, 1]
            for k, p in enumerate(parts):
                hidden = jnp.maximum(pre[8 * h : 8 * h + 8, p], 0.0)
                direction[k] = direction[k] + t0 * hidden
                magnitude[k] = magnitude[k] + t1 * hidden
        direction = jnp.concatenate(direction, axis=1)
        magnitude = jnp.concatenate(magnitude, axis=1)
        w = weight[row0 : row0 + 8, at].astype(jnp.float32)
        out[:, at] = (w - STEP_SCALE * direction * jnp.exp(EXP_SCALE * magnitude)).astype(jnp.bfloat16)

    tiles = out.shape[1] // TILE
    first(0, pre0)

    def two(i, carry):
        first(2 * i + 1, pre1)
        rest(2 * i, pre0)
        first(2 * i + 2, pre0)
        rest(2 * i + 1, pre1)
        return carry

    lax.fori_loop(0, tiles // 2 - 1, two, 0)
    first(tiles - 1, pre1)
    rest(tiles - 2, pre0)
    rest(tiles - 1, pre1)
    for c in copies:
        c.wait()


def here(value):
    return pltpu.with_memory_space_constraint(value, pltpu.VMEM)


def place_kernel(spots, *refs):
    out, sem = refs[-2], refs[-1]
    at = lax.axis_index("fs")
    z, x = at // 4, at % 4
    copies = []
    for ref, where in zip(refs, spots):
        for p, (half, dz, dx) in enumerate(where):
            row = (((z + dz) % 4) * 4 + (x + dx) % 4) * 2 + half
            src = ref if len(where) == 1 else ref.at[p]
            copies.append(pltpu.make_async_copy(src, out.at[row], sem.at[len(copies)]))
            copies[-1].start()
    for c in copies:
        c.wait()


def place(into, pieces, shape):
    ins = [here(p) for p, _ in pieces]
    specs = [pl.BlockSpec(memory_space=pltpu.VMEM)] * len(ins)
    alias = {}
    if into is not None:
        ins.append(into)
        specs.append(pl.BlockSpec(memory_space=pl.ANY))
        alias = {len(ins) - 1: 0}
    spots = [spot for _, spot in pieces]
    return pl.pallas_call(
        lambda *refs: place_kernel(spots, *refs),
        out_shape=jax.ShapeDtypeStruct(shape, jnp.bfloat16),
        in_specs=specs,
        out_specs=pl.BlockSpec(memory_space=pl.ANY),
        scratch_shapes=[pltpu.SemaphoreType.DMA((sum(map(len, spots)),))],
        compiler_params=pltpu.CompilerParams(vmem_limit_bytes=1 << 20),
        input_output_aliases=alias,
    )(*ins)


def moved(value, dz, dx):
    pairs = []
    for z in range(4):
        for x in range(4):
            pairs.append((z * 4 + x, ((z + dz) % 4) * 4 + (x + dx) % 4))
    return lax.ppermute(value, "fs", pairs)


def update_rows(row0, entries, layer, sums, table, columns, gradient, mom_next, second_next, weight):
    width = gradient.shape[1]
    vmem = pl.BlockSpec(memory_space=pltpu.VMEM)
    arrays = [here(v) for v in (sums, table, columns, gradient, mom_next, second_next, weight)]
    outs, out_specs, sems = [pltpu.VMEM((8, width), jnp.bfloat16)], [vmem], []
    if layer is None:
        outs.append(pltpu.VMEM(columns.shape, jnp.bfloat16))
        outs += [jax.ShapeDtypeStruct(v.shape, v.dtype) for v in (mom_next, second_next)]
        out_specs += [vmem] + [pl.BlockSpec(memory_space=pl.ANY)] * 2
        sems = [pltpu.SemaphoreType.DMA((2,))]
    else:
        arrays.append(here(layer))
    return pl.pallas_call(
        lambda *refs: update_kernel(row0, entries, *refs),
        out_shape=tuple(outs),
        in_specs=[vmem] * len(arrays),
        out_specs=tuple(out_specs),
        scratch_shapes=sems + [pltpu.VMEM((columns.shape[0], TILE), jnp.float32)] * 2,
        compiler_params=pltpu.CompilerParams(vmem_limit_bytes=8 << 20),
    )(*arrays)


def per_device(grads, counts, weight, mom, second, in_weight, in_bias, out_weight, out_bias):
    rows, width = mom.shape[1:]
    n_fs = lax.axis_size("fs")
    counts_f = counts.astype(jnp.float32)
    shares = counts_f / jnp.sum(counts_f, axis=0)
    share = lax.dynamic_index_in_dim(shares, lax.axis_index("ep"), 1, keepdims=False)
    n_ep = lax.axis_size("ep")
    came = {}
    ep = lax.axis_index("ep")
    mine = grads[0]
    for slots in SENDS:
        picked = [lax.dynamic_index_in_dim(mine, peer(ep, *slot), 0, keepdims=False) for slot in slots]
        mine, *picked = lax.optimization_barrier((mine, *picked))
        for slot, part in zip(slots, picked):
            pairs = [(i, int(peer(i, *slot))) for i in range(n_ep)]
            came[slot] = part if slot == (0, 0) else lax.ppermute(part, "ep", pairs)
    columns = first_layer_columns(in_weight, in_bias)
    vmem, hbm = pl.BlockSpec(memory_space=pltpu.VMEM), pl.BlockSpec(memory_space=pl.ANY)
    f32 = pltpu.VMEM((rows, width), jnp.float32)
    hid = out_weight.shape[0]
    scalars = jnp.concatenate([share, out_weight.reshape(-1), out_bias])
    small = pl.BlockSpec(memory_space=pltpu.SMEM)
    early, mom_here, second_here, weight_here, table, columns = pl.pallas_call(
        early_kernel,
        out_shape=(
            f32,
            f32,
            f32,
            pltpu.VMEM((rows, width), jnp.bfloat16),
            pltpu.VMEM((hid + 1, 2, 8, LANES), jnp.float32),
            pltpu.VMEM(columns.shape, jnp.float32),
        ),
        in_specs=[small, vmem, hbm, hbm, hbm] + [vmem] * len(EARLY),
        out_specs=(vmem,) * 6,
        scratch_shapes=[pltpu.SemaphoreType.DMA((3,))],
        compiler_params=pltpu.CompilerParams(vmem_limit_bytes=4 << 20),
    )(scalars, columns, mom[0], second[0], weight[0], *[here(came[k]) for k in EARLY])
    gradient, mom_next, second_next, sums = pl.pallas_call(
        moments_kernel,
        out_shape=(f32, f32, f32, pltpu.VMEM((n_fs, 8, LANES), jnp.float32)),
        in_specs=[small] + [vmem] * (3 + len(LATE)),
        out_specs=(vmem,) * 4,
        compiler_params=pltpu.CompilerParams(vmem_limit_bytes=4 << 20),
    )(scalars, *[here(v) for v in (early, mom_here, second_here)], *[here(came[k]) for k in LATE])

    sums = lax.all_to_all(sums, "fs", split_axis=0, concat_axis=0, tiled=True)
    entries = rows * width * n_fs
    args = (entries, sums, table, columns, gradient, mom_next, second_next, weight_here)
    top, layer, mom_next, second_next = update_rows(0, args[0], None, *args[1:])
    (bottom,) = update_rows(8, args[0], layer, *args[1:])

    def go(value, axis, d):
        return moved(value, *(d * a for a in axis))

    halves = ((0, top, (0, 1), (1, 0)), (1, bottom, (1, 0), (0, 1)))
    stages = [[], [], []]
    for half, own, along, across in halves:
        at = lambda i, j: (half, i * along[0] + j * across[0], i * along[1] + j * across[1])
        before = go(own, along, 1)
        after = go(own, along, -1)
        far = go(own, along, 2)
        own_up = go(own, across, 1)
        own_down = go(own, across, -1)
        own_beyond = go(own_down, across, -1)
        three = jnp.stack([before, after, far])
        where = (-1, 1, 2)
        up = go(three, across, 1)
        down = go(three, across, -1)
        beyond_up = go(up[:2], across, 1)
        beyond_down = go(down[2], across, -1)
        spots = lambda j: [at(i, j) for i in where]
        stages[0] += [(own, [at(0, 0)]), (three, spots(0)), (own_up, [at(0, -1)]), (own_down, [at(0, 1)])]
        stages[1] += [(up, spots(-1)), (down, spots(1)), (own_beyond, [at(0, 2)])]
        stages[2] += [(beyond_up, spots(2)[:2]), (beyond_down, spots(2)[2:])]
    shape = (2 * n_fs, 8, width)
    out = None
    for pieces in stages:
        out = place(out, pieces, shape)
    return (out.reshape(1, n_fs * rows, width), mom_next[None], second_next[None])


def solution(mesh):
    in_specs = (
        P("ep", None, "fs", None),
        P(),
        P("ep", "fs", None),
        P("ep", "fs", None),
        P("ep", "fs", None),
        P(),
        P(),
        P(),
        P(),
    )
    out_specs = (P("ep", None, None), P("ep", "fs", None), P("ep", "fs", None))
    return jax.shard_map(per_device, mesh=mesh, in_specs=in_specs, out_specs=out_specs, check_vma=False)
```

```python
import jax
import jax.numpy as jnp
import numpy as np
from jax import lax
from jax.experimental import pallas as pl
from jax.experimental.pallas import tpu as pltpu
from jax.sharding import PartitionSpec as P


MOMENTUM_DECAY = 0.9
SECOND_DECAY = 0.99
NORM_EPS = 1e-06
ROOT_EPS = 1e-08
STEP_SCALE = 0.2
EXP_SCALE = 0.5
LANES = 128
CHUNK = 3584
TILE = 1792


SENDS = [[(2, 0)], [(1, 0), (-1, 0)], [(1, 1), (-1, 1)], [(2, 1), (0, 1), (0, 0)]]
EARLY = [(0, 0), (2, 0), (0, 1), (1, 0), (-1, 0), (1, 1)]
LATE = [(-1, 1), (2, 1)]


def peer(ep, dy, dc, cores=2):
    chips = lax.axis_size("ep") // cores
    return (ep // cores + dy) % chips * cores + (ep % cores + dc) % cores


def weighted_sum(scalars, slots, parts, at, start=None):
    ep = lax.axis_index("ep")
    for (dy, dc), part in zip(slots, parts):
        share = scalars[peer(ep, -dy, dc)]
        term = (share * part[:, at].astype(jnp.float32)).astype(jnp.bfloat16).astype(jnp.float32)
        start = term if start is None else start + term
    return start


def early_kernel(scalars, columns_in, mom, second, weight, *refs):
    parts = refs[: len(EARLY)]
    total, mom_here, second_here, weight_here, table, columns, sem = refs[len(EARLY) :]
    pairs = [(mom, mom_here), (second, second_here), (weight, weight_here)]
    copies = [pltpu.make_async_copy(src, dst, sem.at[k]) for k, (src, dst) in enumerate(pairs)]
    for c in copies:
        c.start()
    first = lax.axis_size("ep")
    for h in range(table.shape[0]):
        for j in range(2):
            table[h, j] = jnp.full((8, LANES), scalars[first + 2 * h + j], jnp.float32)
    columns[...] = columns_in[...]

    def chunk(i, carry):
        at = pl.ds(pl.multiple_of(i * CHUNK, CHUNK), CHUNK)
        total[:, at] = weighted_sum(scalars, EARLY, parts, at)
        return carry

    lax.fori_loop(0, total.shape[1] // CHUNK, chunk, 0)
    for c in copies:
        c.wait()


def folded(squares):
    tiles = [
        squares[r : r + 8, k : k + LANES]
        for k in range(0, squares.shape[1], LANES)
        for r in range(0, squares.shape[0], 8)
    ]
    while len(tiles) > 1:
        tiles = [a + b for a, b in zip(tiles[::2], tiles[1::2])] + tiles[len(tiles) // 2 * 2 :]
    return tiles[0]


def moments_kernel(scalars, early, mom, second, *refs):
    parts = refs[: len(LATE)]
    gradient, mom_next, second_next, sums = refs[len(LATE) :]

    def chunk(i, carry):
        at = pl.ds(pl.multiple_of(i * CHUNK, CHUNK), CHUNK)
        grad = weighted_sum(scalars, LATE, parts, at, early[:, at])
        m = MOMENTUM_DECAY * mom[:, at] + (1.0 - MOMENTUM_DECAY) * grad
        gradient[:, at] = grad
        mom_next[:, at] = m
        second_next[:, at] = SECOND_DECAY * second[:, at] + (1.0 - SECOND_DECAY) * grad * grad
        gg, mm = grad * grad, m * m
        return carry[0] + folded(gg), carry[1] + folded(mm)

    zero = jnp.zeros((8, LANES), jnp.float32)
    a, b = lax.fori_loop(0, gradient.shape[1] // CHUNK, chunk, (zero, zero))
    sums[:, :4] = jnp.full((sums.shape[0], 4, LANES), jnp.sum(a), jnp.float32)
    sums[:, 4:] = jnp.full((sums.shape[0], 4, LANES), jnp.sum(b), jnp.float32)


FEATURE_OF = [0, 1, 2, 3] * 4 + [4, 4]
DEPTH = 8 * len(FEATURE_OF) + 16
CONSTANT_ROWS = [(5, 0), (5, 1), (6, 0), (6, 1)]


def first_layer_columns(in_weight, in_bias):
    feature = np.repeat(np.array(FEATURE_OF), 8)
    sublane = np.arange(feature.size) % 8
    feature = np.concatenate([feature, [f for f, _ in CONSTANT_ROWS]])
    seven = jnp.concatenate([in_weight, in_bias[None]])
    picked = jnp.repeat(seven[feature].T, 8, axis=0)
    mask = (np.arange(picked.shape[0])[:, None] % 8 == sublane[None]).astype(np.float32)
    mask = np.concatenate([mask, np.ones((mask.shape[0], len(CONSTANT_ROWS)), np.float32)], axis=1)
    return jnp.pad(picked * mask, ((0, 0), (0, DEPTH - feature.size)))


def update_kernel(row0, entries, sums, table, columns, gradient, mom, second, weight, *refs):
    hid = table.shape[0] - 1
    pre0, pre1 = refs[-2:]
    copies = []
    if row0 == 0:
        out, layer, mom_out, second_out, sem = refs[:5]
        copies = [pltpu.make_async_copy(mom, mom_out, sem.at[0]), pltpu.make_async_copy(second, second_out, sem.at[1])]
    else:
        layer, out = refs[:2]
    for c in copies:
        c.start()
    if row0 == 0:
        norm = jnp.sqrt(jnp.sum(sums[...], axis=0) / entries + NORM_EPS)
        inv = 1.0 / norm
        lane = lax.broadcasted_iota(jnp.int32, (1, DEPTH), 1)
        group = lane // 8
        paired = group < 16
        const0 = 8 * len(FEATURE_OF)
        is_log = (lane == const0) | (lane == const0 + 1)
        scale = jnp.where(paired & (group % 4 == 0), inv[:1, :1], 1.0)
        scale = jnp.where(paired & (group % 4 == 1), inv[4:5, :1], scale)
        scale = jnp.where(is_log, jnp.log(norm[4:5, :1]), scale)
        low = ((group >= 8) & paired) | (group == 17)
        low = low | ((lane >= const0) & (lane % 2 == 1))
        full = columns[...] * scale
        high = full.astype(jnp.bfloat16).astype(jnp.float32)
        layer[...] = jnp.where(low, full - high, high).astype(jnp.bfloat16)

    def split(pair):
        both = jnp.concatenate(pair, axis=0)
        high = both.astype(jnp.bfloat16)
        return high, (both - high.astype(jnp.float32)).astype(jnp.bfloat16)

    def first(i, pre):
        at = pl.ds(pl.multiple_of(i * TILE, TILE), TILE)
        g, m = gradient[row0 : row0 + 8, at], mom[row0 : row0 + 8, at]
        r = lax.rsqrt(second[row0 : row0 + 8, at] + ROOT_EPS)
        w = weight[row0 : row0 + 8, at].astype(jnp.float32)
        high1, low1 = split([g, m])
        high2, low2 = split([m * r, g * r])
        last = jnp.concatenate([w, w], axis=0).astype(jnp.bfloat16)
        ones = jnp.ones((16, TILE), jnp.bfloat16)
        rows = jnp.concatenate([high1, high2, low1, low2, high1, high2, low1, low2, last, ones], axis=0)
        pre[...] = jnp.dot(layer[...], rows, preferred_element_type=jnp.float32)

    def rest(i, pre):
        at = pl.ds(pl.multiple_of(i * TILE, TILE), TILE)
        parts = [slice(k, k + LANES) for k in range(0, TILE, LANES)]
        direction = [table[hid, 0] for _ in parts]
        magnitude = [table[hid, 1] for _ in parts]
        for h in range(hid):
            t0, t1 = table[h, 0], table[h, 1]
            for k, p in enumerate(parts):
                hidden = jnp.maximum(pre[8 * h : 8 * h + 8, p], 0.0)
                direction[k] = direction[k] + t0 * hidden
                magnitude[k] = magnitude[k] + t1 * hidden
        direction = jnp.concatenate(direction, axis=1)
        magnitude = jnp.concatenate(magnitude, axis=1)
        w = weight[row0 : row0 + 8, at].astype(jnp.float32)
        out[:, at] = (w - STEP_SCALE * direction * jnp.exp(EXP_SCALE * magnitude)).astype(jnp.bfloat16)

    tiles = out.shape[1] // TILE
    first(0, pre0)

    def two(i, carry):
        first(2 * i + 1, pre1)
        rest(2 * i, pre0)
        first(2 * i + 2, pre0)
        rest(2 * i + 1, pre1)
        return carry

    lax.fori_loop(0, tiles // 2 - 1, two, 0)
    first(tiles - 1, pre1)
    rest(tiles - 2, pre0)
    rest(tiles - 1, pre1)
    for c in copies:
        c.wait()


def here(value):
    return pltpu.with_memory_space_constraint(value, pltpu.VMEM)


def place_kernel(spots, *refs):
    out, sem = refs[-2], refs[-1]
    at = lax.axis_index("fs")
    z, x = at // 4, at % 4
    copies = []
    for ref, where in zip(refs, spots):
        for p, (half, dz, dx) in enumerate(where):
            row = (((z + dz) % 4) * 4 + (x + dx) % 4) * 2 + half
            src = ref if len(where) == 1 else ref.at[p]
            copies.append(pltpu.make_async_copy(src, out.at[row], sem.at[len(copies)]))
            copies[-1].start()
    for c in copies:
        c.wait()


def place(into, pieces, shape):
    ins = [here(p) for p, _ in pieces]
    specs = [pl.BlockSpec(memory_space=pltpu.VMEM)] * len(ins)
    alias = {}
    if into is not None:
        ins.append(into)
        specs.append(pl.BlockSpec(memory_space=pl.ANY))
        alias = {len(ins) - 1: 0}
    spots = [spot for _, spot in pieces]
    return pl.pallas_call(
        lambda *refs: place_kernel(spots, *refs),
        out_shape=jax.ShapeDtypeStruct(shape, jnp.bfloat16),
        in_specs=specs,
        out_specs=pl.BlockSpec(memory_space=pl.ANY),
        scratch_shapes=[pltpu.SemaphoreType.DMA((sum(map(len, spots)),))],
        compiler_params=pltpu.CompilerParams(vmem_limit_bytes=1 << 20),
        input_output_aliases=alias,
    )(*ins)


def moved(value, dz, dx):
    pairs = []
    for z in range(4):
        for x in range(4):
            pairs.append((z * 4 + x, ((z + dz) % 4) * 4 + (x + dx) % 4))
    return lax.ppermute(value, "fs", pairs)


def update_rows(row0, entries, layer, sums, table, columns, gradient, mom_next, second_next, weight):
    width = gradient.shape[1]
    vmem = pl.BlockSpec(memory_space=pltpu.VMEM)
    arrays = [here(v) for v in (sums, table, columns, gradient, mom_next, second_next, weight)]
    outs, out_specs, sems = [pltpu.VMEM((8, width), jnp.bfloat16)], [vmem], []
    if layer is None:
        outs.append(pltpu.VMEM(columns.shape, jnp.bfloat16))
        outs += [jax.ShapeDtypeStruct(v.shape, v.dtype) for v in (mom_next, second_next)]
        out_specs += [vmem] + [pl.BlockSpec(memory_space=pl.ANY)] * 2
        sems = [pltpu.SemaphoreType.DMA((2,))]
    else:
        arrays.append(here(layer))
    return pl.pallas_call(
        lambda *refs: update_kernel(row0, entries, *refs),
        out_shape=tuple(outs),
        in_specs=[vmem] * len(arrays),
        out_specs=tuple(out_specs),
        scratch_shapes=sems + [pltpu.VMEM((columns.shape[0], TILE), jnp.float32)] * 2,
        compiler_params=pltpu.CompilerParams(vmem_limit_bytes=8 << 20),
    )(*arrays)


def per_device(grads, counts, weight, mom, second, in_weight, in_bias, out_weight, out_bias):
    rows, width = mom.shape[1:]
    n_fs = lax.axis_size("fs")
    counts_f = counts.astype(jnp.float32)
    shares = counts_f / jnp.sum(counts_f, axis=0)
    share = lax.dynamic_index_in_dim(shares, lax.axis_index("ep"), 1, keepdims=False)
    n_ep = lax.axis_size("ep")
    came = {}
    ep = lax.axis_index("ep")
    mine = grads[0]
    for slots in SENDS:
        picked = [lax.dynamic_index_in_dim(mine, peer(ep, *slot), 0, keepdims=False) for slot in slots]
        mine, *picked = lax.optimization_barrier((mine, *picked))
        for slot, part in zip(slots, picked):
            pairs = [(i, int(peer(i, *slot))) for i in range(n_ep)]
            came[slot] = part if slot == (0, 0) else lax.ppermute(part, "ep", pairs)
    columns = first_layer_columns(in_weight, in_bias)
    vmem, hbm = pl.BlockSpec(memory_space=pltpu.VMEM), pl.BlockSpec(memory_space=pl.ANY)
    f32 = pltpu.VMEM((rows, width), jnp.float32)
    hid = out_weight.shape[0]
    scalars = jnp.concatenate([share, out_weight.reshape(-1), out_bias])
    small = pl.BlockSpec(memory_space=pltpu.SMEM)
    early, mom_here, second_here, weight_here, table, columns = pl.pallas_call(
        early_kernel,
        out_shape=(
            f32,
            f32,
            f32,
            pltpu.VMEM((rows, width), jnp.bfloat16),
            pltpu.VMEM((hid + 1, 2, 8, LANES), jnp.float32),
            pltpu.VMEM(columns.shape, jnp.float32),
        ),
        in_specs=[small, vmem, hbm, hbm, hbm] + [vmem] * len(EARLY),
        out_specs=(vmem,) * 6,
        scratch_shapes=[pltpu.SemaphoreType.DMA((3,))],
        compiler_params=pltpu.CompilerParams(vmem_limit_bytes=4 << 20),
    )(scalars, columns, mom[0], second[0], weight[0], *[here(came[k]) for k in EARLY])
    gradient, mom_next, second_next, sums = pl.pallas_call(
        moments_kernel,
        out_shape=(f32, f32, f32, pltpu.VMEM((n_fs, 8, LANES), jnp.float32)),
        in_specs=[small] + [vmem] * (3 + len(LATE)),
        out_specs=(vmem,) * 4,
        compiler_params=pltpu.CompilerParams(vmem_limit_bytes=4 << 20),
    )(scalars, *[here(v) for v in (early, mom_here, second_here)], *[here(came[k]) for k in LATE])

    sums = lax.all_to_all(sums, "fs", split_axis=0, concat_axis=0, tiled=True)
    entries = rows * width * n_fs
    args = (entries, sums, table, columns, gradient, mom_next, second_next, weight_here)
    top, layer, mom_next, second_next = update_rows(0, args[0], None, *args[1:])
    (bottom,) = update_rows(8, args[0], layer, *args[1:])

    def go(value, axis, d):
        return moved(value, *(d * a for a in axis))

    halves = ((0, top, (0, 1), (1, 0)), (1, bottom, (1, 0), (0, 1)))
    stages = [[], [], [], []]
    for half, own, along, across in halves:
        at = lambda i, j: (half, i * along[0] + j * across[0], i * along[1] + j * across[1])
        before = go(own, along, 1)
        after = go(own, along, -1)
        far = go(own, along, 2)
        own_up = go(own, across, 1)
        own_down = go(own, across, -1)
        own_beyond = go(own_down, across, -1)
        three = jnp.stack([before, after, far])
        where = (-1, 1, 2)
        up = go(three, across, 1)
        down = go(three, across, -1)
        beyond_up = go(up[:2], across, 1)
        beyond_down = go(down[2], across, -1)
        spots = lambda j: [at(i, j) for i in where]
        stages[0] += [(own, [at(0, 0)]), (three, spots(0)), (own_up, [at(0, -1)]), (own_down, [at(0, 1)])]
        stages[1] += [(up, spots(-1)), (down, spots(1)), (own_beyond, [at(0, 2)])]
        stages[2 + half] += [(beyond_up, spots(2)[:2]), (beyond_down, spots(2)[2:])]
    shape = (2 * n_fs, 8, width)
    out = None
    for pieces in stages:
        out = place(out, pieces, shape)
    return (out.reshape(1, n_fs * rows, width), mom_next[None], second_next[None])


def solution(mesh):
    in_specs = (
        P("ep", None, "fs", None),
        P(),
        P("ep", "fs", None),
        P("ep", "fs", None),
        P("ep", "fs", None),
        P(),
        P(),
        P(),
        P(),
    )
    out_specs = (P("ep", None, None), P("ep", "fs", None), P("ep", "fs", None))
    return jax.shard_map(per_device, mesh=mesh, in_specs=in_specs, out_specs=out_specs, check_vma=False)
```
